32 devices in a mesh: row: 4 (over y, core), grid: 8 (over z, x).
Axes of the slice: x: 2, y: 2, z: 4, core: 2. Of those that a mesh axis runs over, the one named last changes fastest.
Arguments:
- h_rows: bfloat16 [8, 1024, 1024], P('grid', 'row'), may hold values from -6 to 6
- x_blocks: bfloat16 [8, 8, 8, 128, 128], P('grid', 'row'), may hold values from -0.1875 to 0.1875
- x_cols: int32 [8, 8, 8], P('grid', 'row'), may hold values from 0 to 7
- sub_blocks: int32 [4, 8, 3, 6], P('row', 'grid'), may hold values from 0 to 7, as said below
- owners: int32 [4, 8, 3], P('row'), may hold values from 0 to 7, as said below
- shift_mu: float32 [1], replicated, may hold values from -4 to 4
- orbitals: bfloat16 [4, 8, 6, 768, 1536], P('row', 'grid'), may hold values from -0.125 to 0.125
Outputs:
- density: float32 [8, 1024], P('grid', 'row')
The draws below stay inside these ranges and needn't reach their ends.
Inputs may be any that keep to these rules, and one draw needn't show every extreme that they name: `x_cols`: entries of a block row may repeat; repeated blocks add. `sub_blocks`: the 6 blocks of a submatrix are distinct; the first is its central block. Within each row index, a device's 3 submatrices go to distinct owners, and every owner receives 1 to 6 submatrices.
All inputs are finite; a program needn't handle non-finite values.
Results may differ from the reference program's by a relative error of at most 0.0003.
Values may be sent and summed in bfloat16 or wider, within the bound.
No kernel may reach another device: no remote copies, remote signals or barrier semaphores. Data moves between devices by JAX's collectives and lax.ppermute only.
A program may use at most 128 MiB of HBM per device.

```python
import jax
import jax.numpy as jnp
from jax import lax

BLK = 128
SUB_BLK = 6
NZ = 8
SUB_DEV = 3
OWN_MAX = 6
PLANE = 256
DEPTH = 4
MARG = 1
ORDER = 768
KB = 8
NREG = 1024
CELLS = 1024
EXT = 1536
N_ROW = 4
N_GRID = 8


owner_table = ((0, 1, 2), (0, 1, 2), (0, 1, 2), (0, 1, 3), (0, 1, 3), (0, 1, 3), (4, 5, 6), (4, 5, 7))


def draw_owners(key, part):

    def single(subkey):
        first, second = jax.random.split(subkey)
        perm_source = jax.random.permutation(first, N_GRID)
        perm_owner = jax.random.permutation(second, N_GRID)
        place = jnp.argsort(perm_source)
        table = jnp.array(owner_table, dtype=jnp.int32)
        within = table[place % 8]
        return perm_owner[(place // 8 * 8)[:, None] + within]
    keys = jax.random.split(jax.random.fold_in(key, 11), N_ROW)
    return jax.vmap(single)(keys).astype(jnp.int32)


def draw_sub_blocks(key, part):
    total = N_ROW * N_GRID * SUB_DEV
    keys = jax.random.split(jax.random.fold_in(key, 23), total)
    picks = jax.vmap(lambda k: jax.random.permutation(k, KB)[:SUB_BLK])(keys)
    return picks.reshape(N_ROW, N_GRID, SUB_DEV, SUB_BLK).astype(jnp.int32)


def with_ends(values, own_key, smallest, high):
    longest = values.shape.index(max(values.shape))
    spots = []
    for shift in (0, 1):
        where = [jax.random.randint(jax.random.fold_in(own_key, axis), (), 0, length) for axis, length in enumerate(values.shape)]
        where[longest] = (where[longest] + shift) % values.shape[longest]
        spots.append(tuple(where))
    return values.at[spots[0]].set(smallest).at[spots[1]].set(high)


def level_of(stream_key, shape, shards, smallest, top_value):
    def one(position, parts):
        heights = jax.random.uniform(jax.random.fold_in(jax.random.fold_in(stream_key, 6), position), (parts,), jnp.float32, smallest / len(shards), top_value / len(shards))
        return jnp.repeat(jnp.exp(heights), shape[position] // parts).reshape((-1,) + (1,) * (len(shape) - position - 1))

    loudness = one(*shards[0])
    for cut in shards[1:]:
        loudness = loudness * one(*cut)
    return loudness


def scatter_about(key, dims, spread, bound, cuts=(), kind=jnp.bfloat16):
    values = spread * jax.random.normal(key, dims, jnp.float32)
    if cuts:
        values = values * level_of(key, dims, cuts, -0.22, 0.18)
    return jnp.clip(values, -bound, bound).astype(kind)


def setup_inputs(seed: int = 0) -> dict:
    splits = jax.random.split(jax.random.key(seed), 8)
    return {
        "h_rows": scatter_about(splits[0], (N_GRID, NREG, NREG), 1.0, 6.0, ((0, 8), (1, 4))),
        "x_blocks": scatter_about(splits[1], (N_GRID, KB, NZ, BLK, BLK), (NZ * BLK) ** -0.5, 0.1875, ((0, 8), (1, 4))),
        "x_cols": with_ends(jax.random.randint(splits[2], (N_GRID, KB, NZ), 0, KB), jax.random.fold_in(splits[2], 1), 0, KB - 1).astype(jnp.int32),
        "sub_blocks": draw_sub_blocks(jax.random.fold_in(splits[7], 71), 0),
        "owners": draw_owners(jax.random.fold_in(splits[7], 71), 0),
        "shift_mu": jnp.clip(jax.random.uniform(splits[5], (1,), jnp.float32, -4.0, 4.0), -4.0, 4.0),
        "orbitals": scatter_about(splits[6], (N_ROW, N_GRID, OWN_MAX, ORDER, EXT), (16 * BLK) ** -0.5, 0.125, ((0, 4), (1, 8))),
    }


def densify(blocks, cols, count):
    onehot = (cols[:, :, None] == jnp.arange(count, dtype=jnp.int32)[None, None, :]).astype(jnp.float32)
    dense = jnp.einsum('rzk,rzab->rakb', onehot, blocks.astype(jnp.float32))
    return dense.reshape(blocks.shape[0] * blocks.shape[2], count * blocks.shape[2]).astype(jnp.bfloat16)

def sign_cols(mat, potential):
    eye = jnp.eye(ORDER, dtype=jnp.float32)
    shifted = mat.astype(jnp.float32) - potential * eye
    scale = jnp.sqrt(jnp.sum(shifted * shifted) / ORDER + 1e-06)
    first = (shifted / (2.0 * scale)).astype(jnp.bfloat16)
    square = jnp.dot(first, first, preferred_element_type=jnp.float32)
    helper = (3.0 * eye - square).astype(jnp.bfloat16)
    second = (0.5 * jnp.dot(first, helper, preferred_element_type=jnp.float32)).astype(jnp.bfloat16)
    square_cols = jnp.dot(second, second[:, :BLK], preferred_element_type=jnp.float32)
    helper_cols = (3.0 * eye[:, :BLK] - square_cols).astype(jnp.bfloat16)
    last = 0.5 * jnp.dot(second, helper_cols, preferred_element_type=jnp.float32)
    return (0.5 * (eye[:, :BLK] - last)).astype(jnp.bfloat16)

def extract(blocks4, picks):
    rows = jnp.take(blocks4, picks, axis=0)
    both = jnp.take(rows, picks, axis=2)
    return both.reshape(ORDER, ORDER)

def reference(h_rows, x_blocks, x_cols, sub_blocks, owners, shift_mu, orbitals):
    potential = shift_mu[0]
    count = x_cols.shape[1]
    subs_by_region = jnp.transpose(sub_blocks, (1, 0, 2, 3))

    def region(item):
        hmat, blocks, cols, picks = item
        dense = densify(blocks, cols, count)
        prod = jnp.dot(dense, hmat, preferred_element_type=jnp.float32).astype(jnp.bfloat16)
        blocks4 = prod.reshape(count, BLK, count, BLK)
        flat = picks.reshape(-1, SUB_BLK)
        result = lax.map(lambda p: sign_cols(extract(blocks4, p), potential), flat)
        return result.reshape(picks.shape[0], picks.shape[1], ORDER, BLK)
    dcols = lax.map(region, (h_rows, x_blocks, x_cols, subs_by_region))
    ngrid = h_rows.shape[0]
    nrow = sub_blocks.shape[0]
    nsub = owners.shape[2]
    pairs_r = jnp.repeat(jnp.arange(nrow, dtype=jnp.int32), ngrid)
    pairs_o = jnp.tile(jnp.arange(ngrid, dtype=jnp.int32), nrow)

    def collocate(item):
        rindex, oindex = item
        table = owners[rindex]
        hit = table == oindex
        has = jnp.any(hit, axis=1)
        which = lax.optimization_barrier(jnp.sum(jnp.arange(nsub, dtype=jnp.int32)[None, :] * hit.astype(jnp.int32), axis=1))
        place = jnp.cumsum(has.astype(jnp.int32)) - 1
        select = has[None, :] & (place[None, :] == jnp.arange(OWN_MAX, dtype=jnp.int32)[:, None])
        selint = select.astype(jnp.int32)
        source = lax.optimization_barrier(jnp.sum(selint * jnp.arange(ngrid, dtype=jnp.int32)[None, :], axis=1))
        slot_k = lax.optimization_barrier(jnp.sum(selint * which[None, :], axis=1))
        live = jnp.any(select, axis=1)
        cols = dcols[source, rindex, slot_k]
        phi = orbitals[rindex, oindex].astype(jnp.float32)
        proj = jnp.einsum('tnm,tnx->tmx', cols.astype(jnp.float32), phi)
        values = lax.optimization_barrier(jnp.sum(proj * phi[:, :BLK, :], axis=1))
        return lax.optimization_barrier(jnp.sum(jnp.where(live[:, None], values, 0.0), axis=0))
    windows = lax.map(collocate, (pairs_r, pairs_o)).reshape(nrow, ngrid, EXT)
    total = lax.optimization_barrier(jnp.sum(windows, axis=0)).reshape(ngrid, DEPTH + 2 * MARG, PLANE)
    core = total[:, MARG:MARG + DEPTH]
    lower = total[:, :MARG]
    upper = total[:, MARG + DEPTH:]
    core = core.at[:, :MARG].add(jnp.roll(upper, 1, axis=0))
    core = core.at[:, DEPTH - MARG:].add(jnp.roll(lower, -1, axis=0))
    return core.reshape(ngrid, CELLS)
```

```python
import jax
import jax.numpy as jnp
from jax import lax
from jax.experimental import pallas as pl
from jax.experimental.pallas import tpu as pltpu
from jax.sharding import PartitionSpec as P

BLK = 128
OWN_MAX = 6
PLANE = 256
DEPTH = 4
MARG = 1
ORDER = 768
SUB_BLK = ORDER // BLK
TILE = 256


def densify(blocks, cols, count):
    onehot = (cols[:, :, None] == jnp.arange(count, dtype=jnp.int32)[None, None, :]).astype(
        jnp.bfloat16
    )
    dense = jnp.einsum("rzk,rzab->rakb", onehot, blocks, preferred_element_type=jnp.float32)
    return dense.reshape(blocks.shape[0] * blocks.shape[2], count * blocks.shape[2]).astype(
        jnp.bfloat16
    )


def across_chips(value, steps):
    count = lax.axis_size("row")
    pairs = [(src, (src + 2 * steps) % count) for src in range(count)]
    return lax.ppermute(value, "row", pairs)


def across_cores(value):
    count = lax.axis_size("row")
    return lax.ppermute(value, "row", [(src, src ^ 1) for src in range(count)])


def eye_tile(rows, cols, row0, col0):
    r = lax.broadcasted_iota(jnp.int32, (rows, cols), 0) + row0
    c = lax.broadcasted_iota(jnp.int32, (rows, cols), 1) + col0
    return r == c


def sign_kernel(srcs, picks, targets, mu, *refs):
    nrow = srcs.shape[0]
    xs = refs[:nrow]
    hs = refs[nrow : 2 * nrow]
    out, prod, shifted, helper, second = refs[2 * nrow :]
    rows = xs[0].shape[0]
    for i in range(nrow):
        acc = None
        for j in range(nrow):
            at = pl.multiple_of(srcs[j] * rows, rows)
            part = jnp.dot(
                xs[i][:, pl.ds(at, rows)], hs[j][...], preferred_element_type=jnp.float32
            )
            acc = part if acc is None else acc + part
        to = pl.multiple_of(srcs[i] * rows, rows)
        prod[pl.ds(to, rows), :] = acc.astype(jnp.bfloat16)
    potential = mu[0]
    for k in range(targets.shape[0]):
        total = jnp.zeros((BLK, BLK), jnp.float32)
        for a in range(SUB_BLK):
            ra = pl.multiple_of(picks[k, a] * BLK, BLK)
            for b in range(SUB_BLK):
                cb = pl.multiple_of(picks[k, b] * BLK, BLK)
                block = prod[pl.ds(ra, BLK), pl.ds(cb, BLK)]
                wide = block.astype(jnp.float32)
                if a == b:
                    wide = jnp.where(eye_tile(BLK, BLK, 0, 0), wide - potential, wide)
                    block = wide.astype(jnp.bfloat16)
                total = total + wide * wide
                shifted[a * BLK : (a + 1) * BLK, b * BLK : (b + 1) * BLK] = block
        norm = jnp.sum(jnp.sum(total, axis=0, keepdims=True), axis=1, keepdims=True)
        half = 0.5 * lax.rsqrt(norm / ORDER + 1e-06)
        for t in range(ORDER // TILE):
            at = slice(t * TILE, (t + 1) * TILE)
            square = jnp.dot(shifted[at, :], shifted[...], preferred_element_type=jnp.float32)
            value = -(half * half) * square
            helper[at, :] = jnp.where(
                eye_tile(TILE, ORDER, t * TILE, 0), value + 3.0, value
            ).astype(jnp.bfloat16)
        for t in range(ORDER // TILE):
            at = slice(t * TILE, (t + 1) * TILE)
            z1 = jnp.dot(shifted[at, :], helper[...], preferred_element_type=jnp.float32)
            second[at, :] = ((0.5 * half) * z1).astype(jnp.bfloat16)
        unit = eye_tile(ORDER, BLK, 0, 0)
        square = jnp.dot(second[...], second[:, :BLK], preferred_element_type=jnp.float32)
        y1 = jnp.where(unit, 3.0 - square, -square).astype(jnp.bfloat16)
        last = -0.25 * jnp.dot(second[...], y1, preferred_element_type=jnp.float32)
        out[targets[k]] = jnp.where(unit, last + 0.5, last).astype(jnp.bfloat16)


def sign_columns(srcs, picks, targets, mu, xs, hs, ngrid):
    nreg = xs[0].shape[1]
    smem = pl.BlockSpec(memory_space=pltpu.SMEM)
    vmem = pl.BlockSpec(memory_space=pltpu.VMEM)
    return pl.pallas_call(
        sign_kernel,
        out_shape=jax.ShapeDtypeStruct((ngrid, ORDER, BLK), jnp.bfloat16),
        in_specs=[smem] * 4 + [vmem] * (2 * len(xs)),
        out_specs=vmem,
        scratch_shapes=[
            pltpu.VMEM((nreg, nreg), jnp.bfloat16),
            pltpu.VMEM((ORDER, ORDER), jnp.bfloat16),
            pltpu.VMEM((ORDER, ORDER), jnp.bfloat16),
            pltpu.VMEM((ORDER, ORDER), jnp.bfloat16),
        ],
        name="sign",
    )(srcs, picks, targets, mu, *xs, *hs)


def window_kernel(source, live, cols, phi, out):
    t = pl.program_id(0)

    @pl.when(t == 0)
    def _():
        out[...] = jnp.zeros_like(out)

    @pl.when(live[t] > 0)
    def _():
        proj = lax.dot_general(
            cols[0], phi[0], (((0,), (0,)), ((), ())), preferred_element_type=jnp.float32
        )
        values = proj * phi[0, :BLK, :].astype(jnp.float32)
        out[...] += jnp.sum(values, axis=0, keepdims=True)


def windows(source, live, incoming, phi):
    own, order, ext = phi.shape
    return pl.pallas_call(
        window_kernel,
        out_shape=jax.ShapeDtypeStruct((1, ext), jnp.float32),
        grid_spec=pltpu.PrefetchScalarGridSpec(
            num_scalar_prefetch=2,
            grid=(own,),
            in_specs=[
                pl.BlockSpec((1, order, BLK), lambda t, source, live: (source[t], 0, 0)),
                pl.BlockSpec((1, order, ext), lambda t, source, live: (t, 0, 0)),
            ],
            out_specs=pl.BlockSpec((1, ext), lambda t, source, live: (0, 0)),
        ),
        name="window",
    )(source, live, incoming, phi)


def on_device(h_rows, x_blocks, x_cols, sub_blocks, owners, shift_mu, orbitals):
    nrow = lax.axis_size("row")
    ngrid = lax.axis_size("grid")
    nchip = nrow // 2
    nreg = h_rows.shape[2]
    count = nreg // BLK
    me = lax.axis_index("row")
    myself = lax.axis_index("grid")

    h_own = h_rows[0]
    x_own = densify(x_blocks[0], x_cols[0], count)
    hs = [h_own] + [across_chips(h_own, s) for s in range(1, nchip)]
    xs = [x_own] + [across_chips(x_own, s) for s in range(1, nchip)]
    hs = hs + [across_cores(v) for v in hs]
    xs = xs + [across_cores(v) for v in xs]
    near = (me - 2 * jnp.arange(nchip, dtype=jnp.int32)) % nrow
    srcs = jnp.concatenate([near, near ^ 1])

    table = owners[0]
    targets = lax.dynamic_index_in_dim(table, myself, 0, keepdims=False)
    outgoing = sign_columns(srcs, sub_blocks[0, 0], targets, shift_mu, xs, hs, ngrid)

    hit = table == myself
    has = jnp.any(hit, axis=1)
    before = jnp.arange(ngrid)[None, :] <= jnp.arange(ngrid)[:, None]
    place = jnp.sum((before & has[None, :]).astype(jnp.int32), axis=1) - 1
    select = has[None, :] & (place[None, :] == jnp.arange(OWN_MAX, dtype=jnp.int32)[:, None])
    selint = select.astype(jnp.int32)
    source = jnp.sum(selint * jnp.arange(ngrid, dtype=jnp.int32)[None, :], axis=1)
    live = jnp.sum(selint, axis=1)

    incoming = lax.all_to_all(outgoing, "grid", split_axis=0, concat_axis=0, tiled=True)
    window = windows(source, live, incoming, orbitals[0, 0])

    cells = DEPTH * PLANE
    chunk = cells // nrow
    edge = MARG * PLANE // chunk
    flat = window.reshape(-1, chunk)
    core = flat[edge : edge + nrow]
    ends = jnp.concatenate(
        [flat[edge + nrow :], jnp.zeros((nrow - 2 * edge, chunk), jnp.float32), flat[:edge]]
    )
    mixed = lax.all_to_all(
        jnp.stack([core, ends], axis=1), "row", split_axis=0, concat_axis=0, tiled=True
    )
    both = jnp.sum(mixed, axis=0)
    pairs = [
        (p * ngrid + o, p * ngrid + (o + step) % ngrid)
        for first, step in ((0, 1), (nrow - edge, -1))
        for p in range(first, first + edge)
        for o in range(ngrid)
    ]
    moved = lax.ppermute(both[1:], ("row", "grid"), pairs)
    return both[:1] + moved


def solution(mesh):
    in_specs = (
        P("grid", "row", None),
        P("grid", "row", None, None, None),
        P("grid", "row", None),
        P("row", "grid", None, None),
        P("row", None, None),
        P(),
        P("row", "grid", None, None, None),
    )
    out_specs = P("grid", "row")
    return jax.shard_map(
        on_device, mesh=mesh, in_specs=in_specs, out_specs=out_specs, check_vma=False
    )
```

```python
import jax
import jax.numpy as jnp
from jax import lax
from jax.experimental import pallas as pl
from jax.experimental.pallas import tpu as pltpu
from jax.sharding import PartitionSpec as P


BLK = 128
PLANE = 256
DEPTH = 4
MARG = 1
ORDER = 768
SUB_BLK = ORDER // BLK


def densify(blocks, cols, count):
    onehot = (cols[:, :, None] == jnp.arange(count, dtype=jnp.int32)[None, None, :]).astype(
        jnp.bfloat16
    )
    dense = jnp.einsum("rzk,rzab->rakb", onehot, blocks, preferred_element_type=jnp.float32)
    return dense.reshape(blocks.shape[0] * blocks.shape[2], count * blocks.shape[2]).astype(
        jnp.bfloat16
    )


def across_chips(value, steps):
    count = lax.axis_size("row")
    pairs = [(src, (src + 2 * steps) % count) for src in range(count)]
    return lax.ppermute(value, "row", pairs)


def across_cores(value):
    return flipped(value, "row", 1)


def flipped(value, axis, mask):
    count = lax.axis_size(axis)
    return lax.ppermute(value, axis, [(src, src ^ mask) for src in range(count)])


def eye_tile(rows, cols):
    r = lax.broadcasted_iota(jnp.int32, (rows, cols), 0)
    c = lax.broadcasted_iota(jnp.int32, (rows, cols), 1)
    return r == c


def wide_dot(a, b):
    return jnp.dot(a, b, preferred_element_type=jnp.float32)


def product_rows(x, srcs, hs, prod, squares, row0, ready=None):
    rows = x.shape[0]
    acc = None
    for j in reversed(range(len(hs))):
        if j == 0 and ready is not None:
            ready()
        at = pl.multiple_of(srcs[j] * rows, rows)
        part = wide_dot(x[:, pl.ds(at, rows)], hs[j][...])
        acc = part if acc is None else acc + part
    acc = acc.astype(jnp.bfloat16)
    prod[row0 : row0 + rows, :] = acc
    for a in range(rows // BLK):
        for b in range(acc.shape[1] // BLK):
            block = acc[a * BLK : (a + 1) * BLK, b * BLK : (b + 1) * BLK].astype(jnp.float32)
            squares[row0 // BLK + a, b] = jnp.sum((block * block).reshape(-1, 8, BLK), axis=0)


def early_kernel(nrow, srcs, *refs):
    hs = refs[:nrow]
    xs = refs[nrow:-2]
    prod, squares = refs[-2:]
    for i, x in enumerate(xs):
        product_rows(x, srcs, hs, prod, squares, i * x.shape[0])


def sign_kernel(nrow, ngrid, nsub, meta, mu, *refs):
    at_picks = nrow
    at_rows = at_picks + nsub * SUB_BLK
    at_shift = at_rows + nsub * SUB_BLK
    srcs = meta
    h_own, *hs = refs[:nrow]
    xa, xb, prod_early, squares_early = refs[nrow : nrow + 4]
    outs = refs[nrow + 4 : nrow + 4 + ngrid]
    prod, squares, shifted, square, column, h_near, sems = refs[nrow + 4 + ngrid :]
    hs = [h_near] + hs
    rows = xa.shape[0]
    early = prod_early.shape[0]
    loads = [
        pltpu.make_async_copy(h_own, h_near, sems.at[0]),
        pltpu.make_async_copy(prod_early, prod.at[pl.ds(0, early)], sems.at[1]),
        pltpu.make_async_copy(squares_early, squares.at[pl.ds(0, early // BLK)], sems.at[2]),
    ]
    for load in loads:
        load.start()

    def ready():
        for load in loads:
            load.wait()

    product_rows(xa, srcs, hs, prod, squares, early, ready)
    product_rows(xb, srcs, hs, prod, squares, early + rows)
    potential = mu[0]
    halves = []
    for k in range(nsub):
        total = jnp.zeros((8, BLK), jnp.float32)
        for a in range(SUB_BLK):
            ra = meta[at_rows + k * SUB_BLK + a]
            for b in range(SUB_BLK):
                cb = meta[at_picks + k * SUB_BLK + b]
                block = prod[
                    pl.ds(pl.multiple_of(ra * BLK, BLK), BLK),
                    pl.ds(pl.multiple_of(cb * BLK, BLK), BLK),
                ]
                if a == b:
                    wide = block.astype(jnp.float32)
                    wide = jnp.where(eye_tile(BLK, BLK), wide - potential, wide)
                    block = wide.astype(jnp.bfloat16)
                    total = total + jnp.sum((wide * wide).reshape(-1, 8, BLK), axis=0)
                else:
                    total = total + squares[ra, cb]
                shifted[k, a * BLK : (a + 1) * BLK, b * BLK : (b + 1) * BLK] = block
        norm = jnp.sum(jnp.sum(total, axis=0, keepdims=True), axis=1, keepdims=True)
        half = 0.5 * lax.rsqrt(norm / ORDER + 1e-06)
        halves.append(half)
        square[k] = ((half * half) * wide_dot(shifted[k], shifted[k])).astype(jnp.bfloat16)
    firsts = []
    for k in range(nsub):
        start = shifted[k, :, :BLK]
        firsts.append(3.0 * start.astype(jnp.float32) - wide_dot(square[k], start))
    seconds = firsts
    for _ in range(2):
        seconds = [
            3.0 * seconds[k] - wide_dot(square[k], seconds[k].astype(jnp.bfloat16))
            for k in range(nsub)
        ]
    unit = jnp.where(eye_tile(ORDER, BLK), 0.5, 0.0)
    for k in range(nsub):
        last = wide_dot(square[k], seconds[k].astype(jnp.bfloat16))
        sign = (0.125 * halves[k]) * (3.0 * firsts[k] - 0.25 * last)
        column[k] = (unit - sign).astype(jnp.bfloat16)
        for s in range(ngrid):

            @pl.when(meta[at_shift + k] == s)
            def _(k=k, s=s):
                outs[s][...] = column[k]


SMEM = pl.BlockSpec(memory_space=pltpu.SMEM)
VMEM = pl.BlockSpec(memory_space=pltpu.VMEM)
HBM = pl.BlockSpec(memory_space=pltpu.HBM)


def grant(count):
    return pltpu.CompilerParams(vmem_limit_bytes=count)


def work(flops):
    return pl.CostEstimate(flops=flops, transcendentals=0, bytes_accessed=flops // 256)


def early_product(srcs, hs, xs):
    rows, nreg = xs[0].shape
    total = rows * len(xs)
    return pl.pallas_call(
        lambda *refs: early_kernel(len(hs), *refs),
        out_shape=(
            jax.ShapeDtypeStruct((total, nreg), jnp.bfloat16),
            jax.ShapeDtypeStruct((total // BLK, nreg // BLK, 8, BLK), jnp.float32),
        ),
        in_specs=[SMEM] + [VMEM] * (len(hs) + len(xs)),
        out_specs=(VMEM, VMEM),
        compiler_params=grant((8 << 20) + 6 * nreg * nreg),
        cost_estimate=work(2 * total * nreg * nreg),
        name="early",
    )(srcs, *hs, *xs)


def sign_columns(meta, mu, hs, xs, prod, squares, ngrid, nsub):
    rows, nreg = xs[0].shape
    return pl.pallas_call(
        lambda *refs: sign_kernel(len(hs), ngrid, nsub, *refs),
        out_shape=[jax.ShapeDtypeStruct((ORDER, BLK), jnp.bfloat16)] * ngrid,
        in_specs=[SMEM] * 2 + [HBM] + [VMEM] * (len(hs) - 1 + len(xs)) + [HBM] * 2,
        out_specs=[VMEM] * ngrid,
        scratch_shapes=[
            pltpu.VMEM((nreg, nreg), jnp.bfloat16),
            pltpu.VMEM((nreg // BLK, nreg // BLK, 8, BLK), jnp.float32),
            pltpu.VMEM((nsub, ORDER, ORDER), jnp.bfloat16),
            pltpu.VMEM((nsub, ORDER, ORDER), jnp.bfloat16),
            pltpu.VMEM((nsub, ORDER, BLK), jnp.bfloat16),
            pltpu.VMEM((rows, nreg), jnp.bfloat16),
            pltpu.SemaphoreType.DMA((3,)),
        ],
        compiler_params=grant((28 << 20) + 6 * nreg * nreg),
        cost_estimate=work(6 * nsub * ORDER**3),
        name="sign",
    )(meta, mu, *hs, *xs, prod, squares)


def collocate(cols, phi, acc):
    proj = lax.dot_general(
        cols, phi, (((0,), (0,)), ((), ())), preferred_element_type=jnp.float32
    )
    values = proj * phi[:BLK, :].astype(jnp.float32)
    acc[...] += jnp.sum(values, axis=0, keepdims=True)


def first_kernel(at, total, meta, orbitals, *refs):
    count = refs[-2].shape[0]
    cols = refs[:count]
    acc, rest, phi, sems = refs[count:]
    live = [meta[at + i] for i in range(total)]
    slots = [meta[at + total + i] for i in range(total)]

    def fetch(i):
        target = phi.at[i] if i < count else rest.at[i - count]
        return pltpu.make_async_copy(orbitals.at[slots[i]], target, sems.at[i])

    for i in range(total):

        @pl.when(live[i] > 0)
        def _(i=i):
            fetch(i).start()

    acc[...] = jnp.zeros_like(acc)
    for i in range(total):

        @pl.when(live[i] > 0)
        def _(i=i):
            fetch(i).wait()
            if i < count:
                collocate(cols[i][...], phi[i], acc)


def next_kernel(at, first, base, meta, before, phi, *refs):
    *cols, acc = refs
    acc[...] = before[...]
    for i in range(len(cols)):

        @pl.when(meta[at + first + i] > 0)
        def _(i=i):
            collocate(cols[i][...], phi[first - base + i], acc)


def last_kernel(at, first, base, count, nrow, edge, meta, before, phi, *refs):
    cols = refs[:count]
    acc = refs[-1]
    outs = refs[count:-1]
    next_kernel(at, first, base, meta, before, phi, *cols, acc)
    me = meta[0]
    chunk = outs[0].shape[1]
    for s in range(nrow // 2):
        for c in range(2):
            peer = me ^ (2 * s + c)
            core = edge + peer
            end = jnp.where(peer < edge, edge + nrow + peer, jnp.maximum(peer - (nrow - edge), 0))
            for i, start in enumerate((core, end)):
                piece = acc[:, pl.ds(pl.multiple_of(start * chunk, chunk), chunk)]
                outs[s][2 * c + i : 2 * c + i + 1, :] = piece


def first_windows(at, total, cols, meta, orbitals):
    shape = orbitals.shape[1:]
    count = len(cols)
    size = shape[0] * shape[1] * 2
    return pl.pallas_call(
        lambda *refs: first_kernel(at, total, *refs),
        out_shape=(
            jax.ShapeDtypeStruct((1, shape[1]), jnp.float32),
            jax.ShapeDtypeStruct((total - count,) + shape, jnp.bfloat16),
        ),
        in_specs=[SMEM, HBM] + [VMEM] * count,
        out_specs=(VMEM, VMEM),
        scratch_shapes=[
            pltpu.VMEM((count,) + shape, jnp.bfloat16),
            pltpu.SemaphoreType.DMA((total,)),
        ],
        compiler_params=grant((6 << 20) + total * size),
        cost_estimate=work(2 * count * BLK * size),
        name="first",
    )(meta, orbitals, *cols)


def next_windows(at, first, base, cols, meta, before, phi):
    return pl.pallas_call(
        lambda *refs: next_kernel(at, first, base, *refs),
        out_shape=jax.ShapeDtypeStruct(before.shape, jnp.float32),
        in_specs=[SMEM] + [VMEM] * (2 + len(cols)),
        out_specs=VMEM,
        compiler_params=grant(18 << 20),
        name="next",
    )(meta, before, phi, *cols)


def last_windows(at, first, base, cols, meta, before, phi, nrow, edge):
    chunk = DEPTH * PLANE // nrow
    return pl.pallas_call(
        lambda *refs: last_kernel(at, first, base, len(cols), nrow, edge, *refs),
        out_shape=[jax.ShapeDtypeStruct((4, chunk), jnp.float32)] * (nrow // 2),
        in_specs=[SMEM] + [VMEM] * (2 + len(cols)),
        out_specs=[VMEM] * (nrow // 2),
        scratch_shapes=[pltpu.VMEM(before.shape, jnp.float32)],
        compiler_params=grant(18 << 20),
        name="last",
    )(meta, before, phi, *cols)


def send_order(ngrid):
    half = ngrid // 2
    near = list(range(2, half)) + [1]
    far = list(range(half, ngrid))
    return far[:1] + near + far[1:]


def on_device(h_rows, x_blocks, x_cols, sub_blocks, owners, shift_mu, orbitals):
    nrow = lax.axis_size("row")
    ngrid = lax.axis_size("grid")
    nchip = nrow // 2
    rows, nreg = h_rows.shape[1:]
    count = nreg // BLK
    me = lax.axis_index("row")
    myself = lax.axis_index("grid")

    h_own = h_rows[0]
    x_own = densify(x_blocks[0], x_cols[0], count)
    hs = []
    for s in range(nchip):
        h = across_chips(h_own, s) if s else h_own
        hs += [h, across_cores(h)]
    xs = []
    for s in range(nchip):
        x = across_chips(x_own, s) if s else x_own
        xs += [x, across_cores(x)]
    order = jnp.arange(nrow, dtype=jnp.int32)
    srcs = (me // 2 * 2 - order // 2 * 2) % nrow + (me + order) % 2

    picks = sub_blocks[0, 0]
    per = rows // BLK
    chip = picks // per
    rowpicks = ((me // 2 - chip // 2) % nchip * 2 + (chip + me) % 2) * per + picks % per

    table = owners[0]
    targets = lax.dynamic_index_in_dim(table, myself, 0, keepdims=False)
    steps = jnp.arange(ngrid, dtype=jnp.int32)
    has = jnp.any(table == myself, axis=1)
    place = jnp.sum(((steps[None, :] < steps[:, None]) & has[None, :]).astype(jnp.int32), axis=1)
    pair = (steps[None, :] == (steps ^ myself)[:, None]) & has[None, :]
    live = jnp.sum(pair.astype(jnp.int32), axis=1)
    slots = jnp.sum(pair.astype(jnp.int32) * place[None, :], axis=1)
    meta = jnp.concatenate(
        [srcs, picks.reshape(-1), rowpicks.reshape(-1), targets ^ myself, live, slots]
    )
    nsub = picks.shape[0]
    at = nrow + 2 * nsub * SUB_BLK + nsub

    prod, squares = early_product(meta, hs, xs[:-2])
    outgoing = sign_columns(meta, shift_mu, hs, xs[-2:], prod, squares, ngrid, nsub)

    arrived = {0: outgoing[0]}
    for s in send_order(ngrid):
        arrived[s] = flipped(outgoing[s], "grid", s)

    edge = MARG * nrow // DEPTH
    cuts = (ngrid - 3, ngrid - 1)
    got = [arrived[s] for s in range(ngrid)]
    partial, phi = first_windows(at, ngrid, got[: cuts[0]], meta, orbitals[0, 0])
    partial = next_windows(
        at, cuts[0], cuts[0], got[cuts[0] : cuts[1]], meta, partial, phi
    )
    parts = last_windows(at, cuts[1], cuts[0], got[cuts[1] :], meta, partial, phi, nrow, edge)
    total = parts[0]
    for s in range(1, nchip):
        total = total + flipped(parts[s], "row", 2 * s)
    both = total[:2] + across_cores(total[2:])
    pairs = [
        (p * ngrid + o, p * ngrid + (o + step) % ngrid)
        for first, step in ((0, 1), (nrow - edge, -1))
        for p in range(first, first + edge)
        for o in range(ngrid)
    ]
    return both[:1] + lax.ppermute(both[1:], ("row", "grid"), pairs)


def solution(mesh):
    in_specs = (
        P("grid", "row", None),
        P("grid", "row", None, None, None),
        P("grid", "row", None),
        P("row", "grid", None, None),
        P("row", None, None),
        P(),
        P("row", "grid", None, None, None),
    )
    out_specs = P("grid", "row")
    return jax.shard_map(
        on_device, mesh=mesh, in_specs=in_specs, out_specs=out_specs, check_vma=False
    )
```

```python
import jax
import jax.numpy as jnp
from jax import lax
from jax.experimental import pallas as pl
from jax.experimental.pallas import tpu as pltpu
from jax.sharding import PartitionSpec as P


BLK = 128
PLANE = 256
DEPTH = 4
MARG = 1
ORDER = 768
SUB_BLK = ORDER // BLK


def densify(blocks, cols, count):
    onehot = (cols[:, :, None] == jnp.arange(count, dtype=jnp.int32)[None, None, :]).astype(
        jnp.bfloat16
    )
    dense = jnp.einsum("rzk,rzab->rakb", onehot, blocks, preferred_element_type=jnp.float32)
    return dense.reshape(blocks.shape[0] * blocks.shape[2], count * blocks.shape[2]).astype(
        jnp.bfloat16
    )


def across_chips(value, steps):
    count = lax.axis_size("row")
    pairs = [(src, (src + 2 * steps) % count) for src in range(count)]
    return lax.ppermute(value, "row", pairs)


def across_cores(value):
    return flipped(value, "row", 1)


def flipped(value, axis, mask):
    count = lax.axis_size(axis)
    return lax.ppermute(value, axis, [(src, src ^ mask) for src in range(count)])


def eye_tile(rows, cols):
    r = lax.broadcasted_iota(jnp.int32, (rows, cols), 0)
    c = lax.broadcasted_iota(jnp.int32, (rows, cols), 1)
    return r == c


def wide_dot(a, b):
    return jnp.dot(a, b, preferred_element_type=jnp.float32)


def thin_dot(a, b):
    half = a.shape[0] // 2
    return jnp.concatenate([wide_dot(a[:half], b), wide_dot(a[half:], b)], axis=0)


def product_rows(x, h, prod, squares, row0):
    rows = x.shape[0]
    acc = wide_dot(x[...], h[...])
    acc = acc.astype(jnp.bfloat16)
    prod[row0 : row0 + rows, :] = acc
    for a in range(rows // BLK):
        for b in range(acc.shape[1] // BLK):
            block = acc[a * BLK : (a + 1) * BLK, b * BLK : (b + 1) * BLK].astype(jnp.float32)
            squares[row0 // BLK + a, b] = jnp.sum((block * block).reshape(-1, 8, BLK), axis=0)


def early_kernel(nrow, srcs, *refs):
    hs = refs[:nrow]
    xs = refs[nrow:-3]
    prod, squares, whole = refs[-3:]
    rows = hs[0].shape[0]
    for j, h in enumerate(hs):
        whole[pl.ds(pl.multiple_of(srcs[j] * rows, rows), rows), :] = h[...]
    for i, x in enumerate(xs):
        product_rows(x, whole, prod, squares, i * rows)


def sign_kernel(nrow, ngrid, nsub, meta, mu, *refs):
    at_picks = nrow
    at_rows = at_picks + nsub * SUB_BLK
    at_shift = at_rows + nsub * SUB_BLK
    whole, prod_early, squares_early, xa, xb = refs[:5]
    outs = refs[5 : 5 + ngrid]
    prod, squares, shifted, square, column, sems = refs[5 + ngrid :]
    rows = xa.shape[0]
    early = prod_early.shape[0]
    loads = [
        pltpu.make_async_copy(prod_early, prod.at[pl.ds(0, early)], sems.at[0]),
        pltpu.make_async_copy(squares_early, squares.at[pl.ds(0, early // BLK)], sems.at[1]),
    ]
    for load in loads:
        load.start()
    product_rows(xa, whole, prod, squares, early)
    product_rows(xb, whole, prod, squares, early + rows)
    for load in loads:
        load.wait()
    potential = mu[0]
    halves = []
    for k in range(nsub):
        total = jnp.zeros((8, BLK), jnp.float32)
        for a in range(SUB_BLK):
            ra = meta[at_rows + k * SUB_BLK + a]
            for b in range(SUB_BLK):
                cb = meta[at_picks + k * SUB_BLK + b]
                block = prod[
                    pl.ds(pl.multiple_of(ra * BLK, BLK), BLK),
                    pl.ds(pl.multiple_of(cb * BLK, BLK), BLK),
                ]
                if a == b:
                    wide = block.astype(jnp.float32)
                    wide = jnp.where(eye_tile(BLK, BLK), wide - potential, wide)
                    block = wide.astype(jnp.bfloat16)
                    total = total + jnp.sum((wide * wide).reshape(-1, 8, BLK), axis=0)
                else:
                    total = total + squares[ra, cb]
                shifted[k, a * BLK : (a + 1) * BLK, b * BLK : (b + 1) * BLK] = block
        norm = jnp.sum(jnp.sum(total, axis=0, keepdims=True), axis=1, keepdims=True)
        half = 0.5 * lax.rsqrt(norm / ORDER + 1e-06)
        halves.append(half)
        square[k] = ((half * half) * wide_dot(shifted[k], shifted[k])).astype(jnp.bfloat16)
    firsts = []
    for k in range(nsub):
        start = shifted[k, :, :BLK]
        firsts.append(3.0 * start.astype(jnp.float32) - thin_dot(square[k], start))
    seconds = firsts
    for _ in range(2):
        seconds = [
            3.0 * seconds[k] - thin_dot(square[k], seconds[k].astype(jnp.bfloat16))
            for k in range(nsub)
        ]
    unit = jnp.where(eye_tile(ORDER, BLK), 0.5, 0.0)
    for k in range(nsub):
        last = thin_dot(square[k], seconds[k].astype(jnp.bfloat16))
        sign = (0.125 * halves[k]) * (3.0 * firsts[k] - 0.25 * last)
        column[k] = (unit - sign).astype(jnp.bfloat16)
        for s in range(ngrid):

            @pl.when(meta[at_shift + k] == s)
            def _(k=k, s=s):
                outs[s][...] = column[k]


SMEM = pl.BlockSpec(memory_space=pltpu.SMEM)
VMEM = pl.BlockSpec(memory_space=pltpu.VMEM)
HBM = pl.BlockSpec(memory_space=pltpu.HBM)


def grant(count):
    return pltpu.CompilerParams(vmem_limit_bytes=count)


def work(flops):
    return pl.CostEstimate(flops=flops, transcendentals=0, bytes_accessed=flops // 256)


def early_product(srcs, hs, xs):
    rows, nreg = xs[0].shape
    total = rows * len(xs)
    return pl.pallas_call(
        lambda *refs: early_kernel(len(hs), *refs),
        out_shape=(
            pltpu.VMEM((total, nreg), jnp.bfloat16),
            pltpu.VMEM((total // BLK, nreg // BLK, 8, BLK), jnp.float32),
            pltpu.VMEM((nreg, nreg), jnp.bfloat16),
        ),
        in_specs=[SMEM] + [VMEM] * (len(hs) + len(xs)),
        out_specs=(VMEM, VMEM, VMEM),
        compiler_params=grant((8 << 20) + 6 * nreg * nreg),
        cost_estimate=work(2 * total * nreg * nreg),
        name="early",
    )(srcs, *hs, *xs)


def sign_columns(meta, mu, whole, prod, squares, xs, nrow, ngrid, nsub):
    nreg = xs[0].shape[1]
    return pl.pallas_call(
        lambda *refs: sign_kernel(nrow, ngrid, nsub, *refs),
        out_shape=[jax.ShapeDtypeStruct((ORDER, BLK), jnp.bfloat16)] * ngrid,
        in_specs=[SMEM] * 2 + [VMEM] * (3 + len(xs)),
        out_specs=[VMEM] * ngrid,
        scratch_shapes=[
            pltpu.VMEM((nreg, nreg), jnp.bfloat16),
            pltpu.VMEM((nreg // BLK, nreg // BLK, 8, BLK), jnp.float32),
            pltpu.VMEM((nsub, ORDER, ORDER), jnp.bfloat16),
            pltpu.VMEM((nsub, ORDER, ORDER), jnp.bfloat16),
            pltpu.VMEM((nsub, ORDER, BLK), jnp.bfloat16),
            pltpu.SemaphoreType.DMA((2,)),
        ],
        compiler_params=grant((28 << 20) + 6 * nreg * nreg),
        cost_estimate=work(6 * nsub * ORDER**3),
        name="sign",
    )(meta, mu, whole, prod, squares, *xs)


def collocate(cols, phi, acc):
    proj = lax.dot_general(
        cols, phi, (((0,), (0,)), ((), ())), preferred_element_type=jnp.float32
    )
    values = proj * phi[:BLK, :].astype(jnp.float32)
    acc[...] += jnp.sum(values, axis=0, keepdims=True)


def first_kernel(at, total, meta, orbitals, *refs):
    count = refs[-2].shape[0]
    cols = refs[:count]
    acc, rest, phi, sems = refs[count:]
    live = [meta[at + i] for i in range(total)]
    slots = [meta[at + total + i] for i in range(total)]

    def fetch(i):
        target = phi.at[i] if i < count else rest.at[i - count]
        return pltpu.make_async_copy(orbitals.at[slots[i]], target, sems.at[i])

    for i in range(total):

        @pl.when(live[i] > 0)
        def _(i=i):
            fetch(i).start()

    acc[...] = jnp.zeros_like(acc)
    for i in range(total):

        @pl.when(live[i] > 0)
        def _(i=i):
            fetch(i).wait()
            if i < count:
                collocate(cols[i][...], phi[i], acc)


def next_kernel(at, first, base, meta, before, phi, *refs):
    *cols, acc = refs
    acc[...] = before[...]
    for i in range(len(cols)):

        @pl.when(meta[at + first + i] > 0)
        def _(i=i):
            collocate(cols[i][...], phi[first - base + i], acc)


def last_kernel(at, first, base, count, nrow, edge, meta, before, phi, *refs):
    cols = refs[:count]
    acc = refs[-1]
    outs = refs[count:-1]
    next_kernel(at, first, base, meta, before, phi, *cols, acc)
    me = meta[0]
    chunk = outs[0].shape[1]
    for s in range(nrow // 2):
        for c in range(2):
            peer = me ^ (2 * s + c)
            upper = peer < edge
            lower = peer >= nrow - edge
            end = jnp.where(upper, edge + nrow + peer, jnp.maximum(peer - (nrow - edge), 0))
            core = acc[:, pl.ds(pl.multiple_of((edge + peer) * chunk, chunk), chunk)]
            ends = acc[:, pl.ds(pl.multiple_of(end * chunk, chunk), chunk)]
            outs[s][c : c + 1, :] = core
            outs[nrow // 2 + s][c : c + 1, :] = jnp.where(upper | lower, ends, 0.0)


def first_windows(at, total, cols, meta, orbitals):
    shape = orbitals.shape[1:]
    count = len(cols)
    size = shape[0] * shape[1] * 2
    return pl.pallas_call(
        lambda *refs: first_kernel(at, total, *refs),
        out_shape=(
            jax.ShapeDtypeStruct((1, shape[1]), jnp.float32),
            jax.ShapeDtypeStruct((total - count,) + shape, jnp.bfloat16),
        ),
        in_specs=[SMEM, HBM] + [VMEM] * count,
        out_specs=(VMEM, VMEM),
        scratch_shapes=[
            pltpu.VMEM((count,) + shape, jnp.bfloat16),
            pltpu.SemaphoreType.DMA((total,)),
        ],
        compiler_params=grant((6 << 20) + total * size),
        cost_estimate=work(2 * count * BLK * size),
        name="first",
    )(meta, orbitals, *cols)


def next_windows(at, first, base, cols, meta, before, phi):
    return pl.pallas_call(
        lambda *refs: next_kernel(at, first, base, *refs),
        out_shape=jax.ShapeDtypeStruct(before.shape, jnp.float32),
        in_specs=[SMEM] + [VMEM] * (2 + len(cols)),
        out_specs=VMEM,
        compiler_params=grant(18 << 20),
        name="next",
    )(meta, before, phi, *cols)


def last_windows(at, first, base, cols, meta, before, phi, nrow, edge):
    chunk = DEPTH * PLANE // nrow
    return pl.pallas_call(
        lambda *refs: last_kernel(at, first, base, len(cols), nrow, edge, *refs),
        out_shape=[jax.ShapeDtypeStruct((2, chunk), jnp.float32)] * nrow,
        in_specs=[SMEM] + [VMEM] * (2 + len(cols)),
        out_specs=[VMEM] * nrow,
        scratch_shapes=[pltpu.VMEM(before.shape, jnp.float32)],
        compiler_params=grant(18 << 20),
        name="last",
    )(meta, before, phi, *cols)


def send_order(ngrid):
    half = ngrid // 2
    near = list(range(2, half)) + [1]
    far = list(range(half, ngrid))
    return far[:1] + near + far[1:]


def on_device(h_rows, x_blocks, x_cols, sub_blocks, owners, shift_mu, orbitals):
    nrow = lax.axis_size("row")
    ngrid = lax.axis_size("grid")
    nchip = nrow // 2
    rows, nreg = h_rows.shape[1:]
    count = nreg // BLK
    me = lax.axis_index("row")
    myself = lax.axis_index("grid")

    h_own = h_rows[0]
    x_own = densify(x_blocks[0], x_cols[0], count)
    hs = []
    for s in range(nchip):
        h = across_chips(h_own, s) if s else h_own
        hs += [h, across_cores(h)]
    xs = []
    for s in range(nchip):
        x = across_chips(x_own, s) if s else x_own
        xs += [x, across_cores(x)]
    order = jnp.arange(nrow, dtype=jnp.int32)
    srcs = (me // 2 * 2 - order // 2 * 2) % nrow + (me + order) % 2

    picks = sub_blocks[0, 0]
    per = rows // BLK
    chip = picks // per
    rowpicks = ((me // 2 - chip // 2) % nchip * 2 + (chip + me) % 2) * per + picks % per

    table = owners[0]
    targets = lax.dynamic_index_in_dim(table, myself, 0, keepdims=False)
    steps = jnp.arange(ngrid, dtype=jnp.int32)
    has = jnp.any(table == myself, axis=1)
    place = jnp.sum(((steps[None, :] < steps[:, None]) & has[None, :]).astype(jnp.int32), axis=1)
    pair = (steps[None, :] == (steps ^ myself)[:, None]) & has[None, :]
    live = jnp.sum(pair.astype(jnp.int32), axis=1)
    slots = jnp.sum(pair.astype(jnp.int32) * place[None, :], axis=1)
    meta = jnp.concatenate(
        [srcs, picks.reshape(-1), rowpicks.reshape(-1), targets ^ myself, live, slots]
    )
    nsub = picks.shape[0]
    at = nrow + 2 * nsub * SUB_BLK + nsub

    prod, squares, whole = early_product(meta, hs, xs[:-2])
    outgoing = sign_columns(
        meta, shift_mu, whole, prod, squares, xs[-2:], nrow, ngrid, nsub
    )

    arrived = {0: outgoing[0]}
    for s in send_order(ngrid):
        arrived[s] = flipped(outgoing[s], "grid", s)

    edge = MARG * nrow // DEPTH
    cuts = (ngrid - 3, ngrid - 1)
    got = [arrived[s] for s in range(ngrid)]
    partial, phi = first_windows(at, ngrid, got[: cuts[0]], meta, orbitals[0, 0])
    partial = next_windows(
        at, cuts[0], cuts[0], got[cuts[0] : cuts[1]], meta, partial, phi
    )
    parts = last_windows(at, cuts[1], cuts[0], got[cuts[1] :], meta, partial, phi, nrow, edge)
    total = parts[0]
    for s in range(1, nchip):
        total = total + flipped(parts[s], "row", 2 * s)
    for j in range(nchip):
        pairs = [
            ((y ^ j) * 2 * ngrid + c * ngrid + o, y * 2 * ngrid + c * ngrid + (o + step) % ngrid)
            for y, step in ((0, 1), (nchip - 1, -1))
            for c in range(2)
            for o in range(ngrid)
        ]
        total = total + lax.ppermute(parts[nchip + j], ("row", "grid"), pairs)
    return total[:1] + across_cores(total[1:])


def solution(mesh):
    in_specs = (
        P("grid", "row", None),
        P("grid", "row", None, None, None),
        P("grid", "row", None),
        P("row", "grid", None, None),
        P("row", None, None),
        P(),
        P("row", "grid", None, None, None),
    )
    out_specs = P("grid", "row")
    return jax.shard_map(
        on_device, mesh=mesh, in_specs=in_specs, out_specs=out_specs, check_vma=False
    )
```
